128 devices in a mesh: row: 2 (over core), col: 64 (over z, y, x).
Axes of the slice: x: 4, y: 4, z: 4, core: 2. Of those that a mesh axis runs over, the one named last changes fastest.
Arguments:
- embeddings: bfloat16 [1024, 4096], P('col', 'row'), may hold values from -6 to 6
- slab_weight: bfloat16 [4096, 131072], P('row', 'col'), may hold values from -0.09375 to 0.09375
- target_table: bfloat16 [256, 131072], P(None, 'col'), may hold values from -6 to 6
- client_ids: int32 [1024], replicated, may hold values from 0 to 255
- client_weights: float32 [1024], replicated, may hold values from 0.1 to 1
Outputs:
- embed_grad: float32 [1024, 4096], P('col', 'row')
- slab_grad: float32 [4096, 131072], P('row', 'col')
The draws below stay inside these ranges and needn't reach their ends.
Inputs may be any that keep to these rules, and one draw needn't show every extreme that they name: `client_ids`: table rows may repeat among clients.
All inputs are finite; a program needn't handle non-finite values.
Results may differ from the reference program's by a relative error of at most 0.0065.
Values may be sent and summed in bfloat16 or wider, within the bound.
No kernel may reach another device: no remote copies, remote signals or barrier semaphores. Data moves between devices by JAX's collectives and lax.ppermute only.
A program may use at most 128 MiB of HBM per device.

```python
import math
import jax
import jax.numpy as jnp
from jax import lax

H = 4096
O = 131072
POOL = 256
B = 1024
N_ROW = 2


def with_ends(result, rng, smallest, largest):
    place = [jax.random.randint(jax.random.fold_in(rng, axis), (), 0, length) for axis, length in enumerate(result.shape)]
    longest = result.shape.index(max(result.shape))
    neighbour = place[:longest] + [(place[longest] + 1) % result.shape[longest]] + place[longest + 1:]
    return result.at[tuple(place)].set(smallest).at[tuple(neighbour)].set(largest)


def level_of(stream_key, dims, pieces, low, high):
    factor_of, own = 1.0, jax.random.fold_in(stream_key, 6)
    for dim, shards_of in pieces:
        draws = jnp.exp(jax.random.uniform(jax.random.fold_in(own, dim), (shards_of,), jnp.float32, low / len(pieces), high / len(pieces)))
        factor_of = factor_of * jnp.repeat(draws, dims[dim] // shards_of).reshape([-1 if axis == dim else 1 for axis in range(len(dims))])
    return factor_of


def gaussian(key, dims, scale, most, cuts=(), held_as=jnp.bfloat16):
    loudness = level_of(key, dims, cuts, -0.22, 0.18) if cuts else 1.0
    array = jax.random.normal(key, dims, jnp.float32) * scale * loudness
    return jnp.minimum(jnp.maximum(array, -most), most).astype(held_as)


def setup_inputs(seed: int = 0) -> dict:
    key_of = jax.random.split(jax.random.key(seed), 6)
    embeddings = gaussian(key_of[0], (B, H), 1.0, 6.0, ((0, 64), (1, 2)))
    slab_weight = gaussian(key_of[1], (H, O), H ** -0.5, 0.09375, ((0, 2), (1, 64)))
    target_table = gaussian(key_of[2], (POOL, O), 1.0, 6.0, ((1, 64),))
    client_ids = with_ends(jax.random.randint(key_of[3], (B,), 0, POOL), jax.random.fold_in(key_of[3], 1), 0, POOL - 1).astype(jnp.int32)
    client_weights = jnp.clip(jnp.exp(jax.random.uniform(key_of[4], (B,), jnp.float32, math.log(0.1), math.log(1.0))), 0.1, 1.0)
    return {"embeddings": embeddings, "slab_weight": slab_weight, "target_table": target_table, "client_ids": client_ids, "client_weights": client_weights}


def reference(embeddings, slab_weight, target_table, client_ids, client_weights):
    block_width = embeddings.shape[1] // N_ROW
    emitted = jnp.zeros((embeddings.shape[0], slab_weight.shape[1]), jnp.float32)
    for group in range(N_ROW):
        partial_value = jnp.dot(embeddings[:, group * block_width:(group + 1) * block_width],
                          slab_weight[group * block_width:(group + 1) * block_width, :],
                          preferred_element_type=jnp.float32)
        rounded = lax.optimization_barrier(partial_value.astype(jnp.bfloat16))
        emitted = emitted + rounded.astype(jnp.float32)
    target = jnp.take(target_table, client_ids.astype(jnp.int32), axis=0).astype(jnp.float32)
    residual = (client_weights[:, None] * (emitted - target)).astype(jnp.bfloat16)
    embed_grad = lax.dot_general(residual, slab_weight, (((1,), (1,)), ((), ())),
                                 preferred_element_type=jnp.float32)
    slab_grad = lax.dot_general(embeddings, residual, (((0,), (0,)), ((), ())),
                                preferred_element_type=jnp.float32)
    return embed_grad, slab_grad
```

```python
import jax
import jax.numpy as jnp
from jax import lax
from jax.experimental import pallas as pl
from jax.experimental.pallas import tpu as pltpu
from jax.sharding import PartitionSpec as P

STRIDE = {"x": 1, "y": 4, "z": 16}
ORDER = (("x", "y", "z"), ("x", "z", "y"))


def hop(value, phase, offset):
    pairs = []
    for core in range(2):
        stride = STRIDE[ORDER[core][phase]]
        for chip in range(64):
            at = (chip // stride) % 4
            to = chip + ((at + offset) % 4 - at) * stride
            pairs.append((core * 64 + chip, core * 64 + to))
    return lax.ppermute(value, ("row", "col"), pairs)


def fetch(value, phase, offset):
    return hop(value, phase, -offset)


def across(value):
    return lax.ppermute(value, "row", [(0, 1), (1, 0)])


def row_order():
    chip = lax.axis_index("col")
    core = lax.axis_index("row")
    ks = lax.broadcasted_iota(jnp.int32, (64,), 0)
    k3, k2, k1 = ks // 16, (ks // 4) % 4, ks % 4
    dz = jnp.where(core == 0, k3, k2)
    dy = jnp.where(core == 0, k2, k3)
    z, y, x = chip // 16, (chip // 4) % 4, chip % 4
    return ((z + dz) % 4) * 16 + ((y + dy) % 4) * 4 + (x + k1) % 4


def residual_kernel(own_ref, r0_ref, r1_ref, r2_ref, r3_ref, out_ref):
    step = own_ref.shape[0] // 4
    for q, ref in enumerate((r0_ref, r1_ref, r2_ref, r3_ref)):
        span = slice(q * step, (q + 1) * step)
        both = own_ref[span, :].astype(jnp.float32) + ref[0].astype(jnp.float32)
        out_ref[span, :] = both.astype(jnp.bfloat16)


def residual_plane(k, own, others):
    rows, width = own.shape
    cols = 1024
    theirs = pl.BlockSpec((1, rows // 4, cols), lambda j: (k, 0, j))
    return pl.pallas_call(
        residual_kernel,
        grid=(width // cols,),
        in_specs=[pl.BlockSpec((rows, cols), lambda j: (0, j)), theirs, theirs, theirs, theirs],
        out_specs=pl.BlockSpec((rows, cols), lambda j: (0, j)),
        out_shape=jax.ShapeDtypeStruct((rows, width), jnp.bfloat16),
        compiler_params=pltpu.CompilerParams(vmem_limit_bytes=8 * 2**20),
        cost_estimate=pl.CostEstimate(flops=rows * width * 64, bytes_accessed=3 * 2**20, transcendentals=0),
        name="residual",
    )(own, *others)


def slab_kernel(e0, e1, e2, e3, r0, r1, r2, r3, out_ref, e_all, r_all):
    step = e0.shape[0]

    @pl.when(pl.program_id(0) == 0)
    def _():
        for q, ref in enumerate((r0, r1, r2, r3)):
            r_all[q * step : (q + 1) * step, :] = ref[...]

    for q, ref in enumerate((e0, e1, e2, e3)):
        e_all[q * step : (q + 1) * step, :] = ref[...]
    out_ref[...] = lax.dot_general(
        e_all[...], r_all[...], (((0,), (0,)), ((), ())), preferred_element_type=jnp.float32
    )


def slab_product(planes, residuals):
    rows, hidden = planes[0].shape
    width = residuals[0].shape[1]
    block = 256
    return pl.pallas_call(
        slab_kernel,
        grid=(hidden // block,),
        in_specs=[pl.BlockSpec((rows, block), lambda i: (0, i))] * 4 + [pl.BlockSpec((rows, width), lambda i: (0, 0))] * 4,
        out_specs=pl.BlockSpec((block, width), lambda i: (i, 0)),
        out_shape=jax.ShapeDtypeStruct((hidden, width), jnp.float32),
        scratch_shapes=[pltpu.VMEM((4 * rows, block), jnp.bfloat16), pltpu.VMEM((4 * rows, width), jnp.bfloat16)],
        compiler_params=pltpu.CompilerParams(dimension_semantics=("arbitrary",), vmem_limit_bytes=40 * 2**20),
        cost_estimate=pl.CostEstimate(
            flops=8 * rows * hidden * width, bytes_accessed=24 * 2**20, transcendentals=0
        ),
        name="slab_grad",
    )(*planes, *residuals)


def per_device(embeddings, slab_weight, target_table, client_ids, client_weights):
    value = embeddings
    for phase in range(2):
        value = jnp.stack([value, *(fetch(value, phase, k) for k in (1, 2, 3))])
        value = value.reshape(-1, value.shape[-1])
    rows = value.shape[0]
    planes = {0: value}
    for k in (1, 3):
        planes[k] = fetch(value, 2, k)
    upper = fetch(planes[1][: rows // 2], 2, 1)
    lower = fetch(planes[3][rows // 2 :], 2, 3)
    planes[2] = jnp.concatenate([upper, lower])
    block = row_order()
    ids = client_ids.reshape(64, 16)[block].reshape(-1)
    weights = client_weights.reshape(64, 16)[block].reshape(4, rows)
    picks = (ids[:, None] == lax.broadcasted_iota(jnp.int32, (1, target_table.shape[0]), 1)).astype(jnp.bfloat16)
    target = jnp.dot(picks, target_table, preferred_element_type=jnp.float32).astype(jnp.bfloat16)
    target, weights = lax.optimization_barrier((target, weights))
    target = target.reshape(4, rows, -1)
    partial, other = {}, {}
    for k in (0, 1, 3, 2):
        part = jnp.dot(planes[k], slab_weight, preferred_element_type=jnp.float32)
        part = weights[k][:, None] * (part - 0.5 * target[k].astype(jnp.float32))
        partial[k] = part.astype(jnp.bfloat16)
        other[k] = across(partial[k])
    others = [other[k].reshape(4, rows // 4, -1) for k in range(4)]
    residual, sent = {}, {}
    for k in (2, 1, 3, 0):
        residual[k] = residual_plane(k, partial[k], others)
        part = lax.dot_general(residual[k], slab_weight, (((1,), (1,)), ((), ())), preferred_element_type=jnp.float32)
        part = part.astype(jnp.bfloat16) if k else lax.optimization_barrier(part)
        sent[k] = hop(part, 2, k) if k else part
    slab_grad = slab_product([planes[k] for k in range(4)], [residual[k] for k in range(4)])
    total = sum(sent[k].astype(jnp.float32) for k in range(4))
    for phase in (1, 0):
        cut = total.reshape(4, -1, total.shape[-1])
        total = cut[0] + sum(hop(cut[k].astype(jnp.bfloat16), phase, k).astype(jnp.float32) for k in (1, 2, 3))
    return total, slab_grad


def solution(mesh):
    placed = (P("col", "row"), P("row", "col"), P(None, "col"), P(), P())
    return jax.shard_map(
        per_device,
        mesh=mesh,
        in_specs=placed,
        out_specs=(P("col", "row"), P("row", "col")),
        check_vma=False,
    )
```

```python
import jax
import jax.numpy as jnp
from jax import lax
from jax.experimental import pallas as pl
from jax.experimental.pallas import tpu as pltpu
from jax.sharding import PartitionSpec as P

STRIDE = {"x": 1, "y": 4, "z": 16}
ORDER = (("x", "y", "z"), ("x", "z", "y"))
SLAB_CUTS = (4, 4)


def hop(value, phase, offset):
    pairs = []
    for core in range(2):
        stride = STRIDE[ORDER[core][phase]]
        for chip in range(64):
            at = (chip // stride) % 4
            to = chip + ((at + offset) % 4 - at) * stride
            pairs.append((core * 64 + chip, core * 64 + to))
    return lax.ppermute(value, ("row", "col"), pairs)


def fetch(value, phase, offset):
    return hop(value, phase, -offset)


def across(value):
    return lax.ppermute(value, "row", [(0, 1), (1, 0)])


def joined(*pieces):
    return jnp.stack(pieces).reshape(-1, pieces[0].shape[1])


def row_order():
    chip = lax.axis_index("col")
    core = lax.axis_index("row")
    ks = lax.broadcasted_iota(jnp.int32, (64,), 0)
    k3, k2, k1 = ks // 16, (ks // 4) % 4, ks % 4
    dz = jnp.where(core == 0, k3, k2)
    dy = jnp.where(core == 0, k2, k3)
    z, y, x = chip // 16, (chip // 4) % 4, chip % 4
    return ((z + dz) % 4) * 16 + ((y + dy) % 4) * 4 + (x + k1) % 4


def place(k3, k2):
    if k3 == 0:
        return 0, k2
    if k3 == 2:
        return (3, k2) if k2 < 2 else (4, k2 - 2)
    return (1 if k2 < 2 else 2), (0 if k3 == 1 else 2) + k2 % 2


EARLY = [(2, 0), (2, 1), (3, 0), (3, 1), *((1, k) for k in range(4)), *((0, k) for k in range(4))]
LATE = [(2, 2), (2, 3), (3, 2), (3, 3)]


def residual_kernel(blocks, used, *refs):
    *refs, out_ref = refs
    own = dict(zip(used, refs[: len(used)]))
    theirs = dict(zip(used, refs[len(used) :]))
    for row, (k3, k2) in enumerate(blocks):
        group, at = place(k3, k2)
        mine = own[group][at * 64 : (at + 1) * 64, :].astype(jnp.float32)
        group, at = place(k2, k3)
        both = mine + theirs[group][at * 64 : (at + 1) * 64, :].astype(jnp.float32)
        out_ref[row * 64 : (row + 1) * 64, :] = both.astype(jnp.bfloat16)


def residual_of(blocks, used, own, theirs):
    width = own[0].shape[1]
    cols = width // 4
    groups = [own[g] for g in used] + [theirs[g] for g in used]
    return pl.pallas_call(
        lambda *refs: residual_kernel(blocks, used, *refs),
        grid=(width // cols,),
        in_specs=[pl.BlockSpec((g.shape[0], cols), lambda j: (0, j)) for g in groups],
        out_specs=pl.BlockSpec((64 * len(blocks), cols), lambda j: (0, j)),
        out_shape=jax.ShapeDtypeStruct((64 * len(blocks), width), jnp.bfloat16),
        compiler_params=pltpu.CompilerParams(vmem_limit_bytes=10 * 2**20),
        cost_estimate=pl.CostEstimate(
            flops=64 * 64 * len(blocks) * width, bytes_accessed=6 * 64 * len(blocks) * width, transcendentals=0
        ),
        name="residual",
    )(*groups)


def slab_kernel(count, *refs):
    e_refs, early_ref, late_ref = refs[:count], refs[count], refs[count + 1]
    out_ref, e_early, e_late = refs[-3:]
    row = 0
    rows = early_ref.shape[0]
    for ref in e_refs:
        size = ref.shape[0]
        if row < rows:
            e_early[row : row + size, :] = ref[...]
        else:
            e_late[row - rows : row - rows + size, :] = ref[...]
        row += size
    dims = (((0,), (0,)), ((), ()))
    out_ref[...] = lax.dot_general(
        e_early[...], early_ref[...], dims, preferred_element_type=jnp.float32
    ) + lax.dot_general(e_late[...], late_ref[...], dims, preferred_element_type=jnp.float32)


def slab_product(pieces, early, late, whole, first, count):
    hidden = pieces[0].shape[1]
    width = early.shape[1]
    rows = early.shape[0] + late.shape[0]
    block = hidden // 8
    given = () if whole is None else (whole,)
    return pl.pallas_call(
        lambda *refs: slab_kernel(len(pieces), *refs),
        grid=(count,),
        in_specs=[pl.BlockSpec((p.shape[0], block), lambda i: (0, first + i)) for p in pieces]
        + [pl.BlockSpec(r.shape, lambda i: (0, 0), pipeline_mode=pl.Buffered(1)) for r in (early, late)]
        + [pl.BlockSpec(memory_space=pl.ANY)] * len(given),
        out_specs=pl.BlockSpec((block, width), lambda i: (first + i, 0)),
        out_shape=jax.ShapeDtypeStruct((hidden, width), jnp.float32),
        scratch_shapes=[
            pltpu.VMEM((early.shape[0], block), jnp.bfloat16),
            pltpu.VMEM((late.shape[0], block), jnp.bfloat16),
        ],
        input_output_aliases={len(pieces) + 2: 0} if given else {},
        compiler_params=pltpu.CompilerParams(dimension_semantics=("arbitrary",), vmem_limit_bytes=20 * 2**20),
        cost_estimate=pl.CostEstimate(
            flops=2 * rows * block * count * width, bytes_accessed=count * 5 * 2**19 + 2**22, transcendentals=0
        ),
        name="slab_grad",
    )(*pieces, early, late, *given)


def stage_kernel(source_ref, out_ref, sem):
    copy = pltpu.make_async_copy(source_ref, out_ref, sem)
    copy.start()
    copy.wait()


def staged(value):
    return pl.pallas_call(
        stage_kernel,
        in_specs=[pl.BlockSpec(memory_space=pltpu.HBM)],
        out_specs=pl.BlockSpec(memory_space=pltpu.VMEM),
        out_shape=pltpu.VMEM(value.shape, value.dtype),
        scratch_shapes=[pltpu.SemaphoreType.DMA],
        compiler_params=pltpu.CompilerParams(vmem_limit_bytes=2**20),
        cost_estimate=pl.CostEstimate(flops=64 * value.size, bytes_accessed=2 * value.size, transcendentals=0),
        name="bring_in",
    )(value)


def times_transpose(name, rows, slab_weight):
    part = lax.dot_general(
        rows, slab_weight, (((1,), (1,)), ((), ())), preferred_element_type=jnp.float32
    )
    return lax.optimization_barrier(part if name == "back0" else part.astype(jnp.bfloat16))


def plus(mine, came):
    return (mine.astype(jnp.float32) + came.astype(jnp.float32)).astype(jnp.bfloat16)


def body(embeddings, slab_weight, target_table, client_ids, client_weights):
    block = row_order()
    ids = client_ids.reshape(64, 16)[block].reshape(-1)
    weights = client_weights.reshape(64, 16)[block].reshape(-1)
    picks = (ids[:, None] == lax.broadcasted_iota(jnp.int32, (1, target_table.shape[0]), 1)).astype(jnp.bfloat16)
    picks, weights = lax.optimization_barrier((picks, weights))
    slab_weight = staged(slab_weight)

    nearby = staged(embeddings)
    value = joined(nearby, *(fetch(embeddings, 0, k) for k in (1, 2, 3)))
    ring = [value, *(fetch(value, 1, k) for k in (1, 2, 3))]
    top, low = joined(*ring[:2]), joined(*ring[2:])
    half = top.shape[0]
    top1 = fetch(top, 2, 1)
    top3 = fetch(top, 2, 3)
    low3 = fetch(low, 2, 3)
    low1 = fetch(low, 2, 1)
    top2 = fetch(top1, 2, 1)
    low2 = fetch(low3, 2, 3)
    target = jnp.dot(picks, target_table, preferred_element_type=jnp.float32).astype(jnp.bfloat16)
    target = lax.optimization_barrier(target)

    groups = [joined(*ring), joined(top1, top3), joined(low1, low3), top2, low2]
    own, theirs = [], []
    for g, rows in enumerate(groups):
        spans = {0: (0,), 1: (2, 6), 2: (3, 7), 3: (4,), 4: (5,)}[g]
        size = rows.shape[0] // len(spans)
        scale = jnp.concatenate([weights[s * half : s * half + size] for s in spans])[:, None]
        wanted = jnp.concatenate([target[s * half : s * half + size] for s in spans])
        part = jnp.dot(rows, slab_weight, preferred_element_type=jnp.float32)
        own.append((scale * (part - 0.5 * wanted.astype(jnp.float32))).astype(jnp.bfloat16))
        theirs.append(across(own[g]))

    early = residual_of(EARLY, (0, 1, 2, 3), own, theirs)
    back_a = times_transpose("back_a", early[: 2 * half], slab_weight)
    far_top = hop(back_a[:half], 2, 3)
    back1 = times_transpose("back1", early[2 * half : 4 * half], slab_weight)
    back0 = times_transpose("back0", early[4 * half :], slab_weight)
    late = residual_of(LATE, (2, 4), own, theirs)
    back_b = times_transpose("back_b", late, slab_weight)
    far_low = hop(back_b[:half], 2, 1)
    low_from3 = hop(back_b[half:], 2, 3)
    top_from1 = hop(back1[:half], 2, 1)
    top_from3 = hop(plus(back_a[half:], far_top), 2, 3)
    low_from1 = hop(plus(back1[half:], far_low), 2, 1)

    pieces = [top2, top3, top1, low1, groups[0], low2, low3]
    slab_grad, first = None, 0
    for count in SLAB_CUTS:
        slab_grad = slab_product(pieces, early, late, slab_grad, first, count)
        first += count

    total = jnp.concatenate(
        [
            back0[:half] + top_from1.astype(jnp.float32) + top_from3.astype(jnp.float32),
            back0[half:] + low_from1.astype(jnp.float32) + low_from3.astype(jnp.float32),
        ]
    )
    for phase in (1, 0):
        cut = total.reshape(4, -1, total.shape[-1])
        total = cut[0]
        for k in (1, 2, 3):
            total = total + hop(cut[k].astype(jnp.bfloat16), phase, k).astype(jnp.float32)
    return total, slab_grad


def solution(mesh):
    placed = (P("col", "row"), P("row", "col"), P(None, "col"), P(), P())
    return jax.shard_map(
        body,
        mesh=mesh,
        in_specs=placed,
        out_specs=(P("col", "row"), P("row", "col")),
        check_vma=False,
    )
```

```python
import jax
import jax.numpy as jnp
from jax import lax
from jax.experimental import pallas as pl
from jax.experimental.pallas import tpu as pltpu
from jax.sharding import PartitionSpec as P

STRIDE = {"x": 1, "y": 4, "z": 16}
ORDER = (("z", "x", "y"), ("z", "y", "x"))
SLAB_CUTS = (5, 3)


def hop(value, phase, offset):
    pairs = []
    for core in range(2):
        stride = STRIDE[ORDER[core][phase]]
        for chip in range(64):
            at = (chip // stride) % 4
            to = chip + ((at + offset) % 4 - at) * stride
            pairs.append((core * 64 + chip, core * 64 + to))
    return lax.ppermute(value, ("row", "col"), pairs)


def fetch(value, phase, offset):
    return hop(value, phase, -offset)


def across(value):
    return lax.ppermute(value, "row", [(0, 1), (1, 0)])


def joined(*pieces):
    return jnp.stack(pieces).reshape(-1, pieces[0].shape[1])


def row_order():
    chip = lax.axis_index("col")
    core = lax.axis_index("row")
    ks = lax.broadcasted_iota(jnp.int32, (64,), 0)
    k3, k2, k1 = ks // 16, (ks // 4) % 4, ks % 4
    block = 0
    for axis, stride in STRIDE.items():
        first, second = (dict(zip(axes, (k1, k2, k3)))[axis] for axes in ORDER)
        at = (chip // stride) % 4
        block = block + ((at + jnp.where(core == 0, first, second)) % 4) * stride
    return block


def place(k3, k2):
    if k3 == 0:
        return 0, k2
    if k3 == 2:
        return (3, k2) if k2 < 2 else (4, k2 - 2)
    return (1 if k2 < 2 else 2), (0 if k3 == 1 else 2) + k2 % 2


EARLY = [(2, 0), (2, 1), (3, 0), (3, 1), *((1, k) for k in range(4)), *((0, k) for k in range(4))]
LATE = [(2, 2), (2, 3), (3, 2), (3, 3)]


def residual_kernel(blocks, used, *refs):
    *refs, out_ref = refs
    own = dict(zip(used, refs[: len(used)]))
    theirs = dict(zip(used, refs[len(used) :]))
    for row, (k3, k2) in enumerate(blocks):
        group, at = place(k3, k2)
        mine = own[group][at * 64 : (at + 1) * 64, :].astype(jnp.float32)
        group, at = place(k2, k3)
        both = mine + theirs[group][at * 64 : (at + 1) * 64, :].astype(jnp.float32)
        out_ref[row * 64 : (row + 1) * 64, :] = both.astype(jnp.bfloat16)


def residual_of(blocks, used, own, theirs):
    width = own[0].shape[1]
    cols = width // 4
    groups = [own[g] for g in used] + [theirs[g] for g in used]
    return pl.pallas_call(
        lambda *refs: residual_kernel(blocks, used, *refs),
        grid=(width // cols,),
        in_specs=[pl.BlockSpec((g.shape[0], cols), lambda j: (0, j)) for g in groups],
        out_specs=pl.BlockSpec((64 * len(blocks), cols), lambda j: (0, j)),
        out_shape=jax.ShapeDtypeStruct((64 * len(blocks), width), jnp.bfloat16),
        compiler_params=pltpu.CompilerParams(vmem_limit_bytes=10 * 2**20),
        cost_estimate=pl.CostEstimate(
            flops=64 * 64 * len(blocks) * width, bytes_accessed=6 * 64 * len(blocks) * width, transcendentals=0
        ),
        name="residual",
    )(*groups)


def slab_kernel(count, *refs):
    e_refs, early_ref, late_ref = refs[:count], refs[count], refs[count + 1]
    out_ref, e_early, e_late = refs[-3:]
    row = 0
    rows = early_ref.shape[0]
    for ref in e_refs:
        size = ref.shape[0]
        if row < rows:
            e_early[row : row + size, :] = ref[...]
        else:
            e_late[row - rows : row - rows + size, :] = ref[...]
        row += size
    dims = (((0,), (0,)), ((), ()))
    out_ref[...] = lax.dot_general(
        e_early[...], early_ref[...], dims, preferred_element_type=jnp.float32
    ) + lax.dot_general(e_late[...], late_ref[...], dims, preferred_element_type=jnp.float32)


def slab_product(pieces, early, late, whole, first, count):
    hidden = pieces[0].shape[1]
    width = early.shape[1]
    rows = early.shape[0] + late.shape[0]
    block = hidden // 8
    given = () if whole is None else (whole,)
    return pl.pallas_call(
        lambda *refs: slab_kernel(len(pieces), *refs),
        grid=(count,),
        in_specs=[pl.BlockSpec((p.shape[0], block), lambda i: (0, first + i)) for p in pieces]
        + [pl.BlockSpec(r.shape, lambda i: (0, 0), pipeline_mode=pl.Buffered(1)) for r in (early, late)]
        + [pl.BlockSpec(memory_space=pl.ANY)] * len(given),
        out_specs=pl.BlockSpec((block, width), lambda i: (first + i, 0)),
        out_shape=jax.ShapeDtypeStruct((hidden, width), jnp.float32),
        scratch_shapes=[
            pltpu.VMEM((early.shape[0], block), jnp.bfloat16),
            pltpu.VMEM((late.shape[0], block), jnp.bfloat16),
        ],
        input_output_aliases={len(pieces) + 2: 0} if given else {},
        compiler_params=pltpu.CompilerParams(dimension_semantics=("arbitrary",), vmem_limit_bytes=20 * 2**20),
        cost_estimate=pl.CostEstimate(
            flops=2 * rows * block * count * width, bytes_accessed=count * 5 * 2**19 + 2**22, transcendentals=0
        ),
        name="slab_grad",
    )(*pieces, early, late, *given)


def stage_kernel(source_ref, out_ref, sem):
    copy = pltpu.make_async_copy(source_ref, out_ref, sem)
    copy.start()
    copy.wait()


def staged(value):
    return pl.pallas_call(
        stage_kernel,
        in_specs=[pl.BlockSpec(memory_space=pltpu.HBM)],
        out_specs=pl.BlockSpec(memory_space=pltpu.VMEM),
        out_shape=pltpu.VMEM(value.shape, value.dtype),
        scratch_shapes=[pltpu.SemaphoreType.DMA],
        compiler_params=pltpu.CompilerParams(vmem_limit_bytes=2**20),
        cost_estimate=pl.CostEstimate(flops=64 * value.size, bytes_accessed=2 * value.size, transcendentals=0),
        name="bring_in",
    )(value)


def times_transpose(name, rows, slab_weight):
    part = lax.dot_general(
        rows, slab_weight, (((1,), (1,)), ((), ())), preferred_element_type=jnp.float32
    )
    return lax.optimization_barrier(part if name == "back0" else part.astype(jnp.bfloat16))


def plus(mine, came):
    return (mine.astype(jnp.float32) + came.astype(jnp.float32)).astype(jnp.bfloat16)


def body(embeddings, slab_weight, target_table, client_ids, client_weights):
    block = row_order()
    ids = client_ids.reshape(64, 16)[block].reshape(-1)
    weights = client_weights.reshape(64, 16)[block].reshape(-1)
    picks = (ids[:, None] == lax.broadcasted_iota(jnp.int32, (1, target_table.shape[0]), 1)).astype(jnp.bfloat16)
    picks, weights = lax.optimization_barrier((picks, weights))
    slab_weight = staged(slab_weight)

    nearby = staged(embeddings)
    value = joined(nearby, *(fetch(embeddings, 0, k) for k in (1, 2, 3)))
    ring = [value, *(fetch(value, 1, k) for k in (1, 2, 3))]
    top, low = joined(*ring[:2]), joined(*ring[2:])
    half = top.shape[0]
    top1 = fetch(top, 2, 1)
    top3 = fetch(top, 2, 3)
    low3 = fetch(low, 2, 3)
    low1 = fetch(low, 2, 1)
    top2 = fetch(top1, 2, 1)
    low2 = fetch(low3, 2, 3)
    target = jnp.dot(picks, target_table, preferred_element_type=jnp.float32).astype(jnp.bfloat16)
    target = lax.optimization_barrier(target)

    groups = [joined(*ring), joined(top1, top3), joined(low1, low3), top2, low2]
    own, theirs = [], []
    for g, rows in enumerate(groups):
        spans = {0: (0,), 1: (2, 6), 2: (3, 7), 3: (4,), 4: (5,)}[g]
        size = rows.shape[0] // len(spans)
        scale = jnp.concatenate([weights[s * half : s * half + size] for s in spans])[:, None]
        wanted = jnp.concatenate([target[s * half : s * half + size] for s in spans])
        part = jnp.dot(rows, slab_weight, preferred_element_type=jnp.float32)
        own.append((scale * (part - 0.5 * wanted.astype(jnp.float32))).astype(jnp.bfloat16))
        theirs.append(across(own[g]))

    early = residual_of(EARLY, (0, 1, 2, 3), own, theirs)
    back_a = times_transpose("back_a", early[: 2 * half], slab_weight)
    far_top = hop(back_a[:half], 2, 3)
    back1 = times_transpose("back1", early[2 * half : 4 * half], slab_weight)
    back0 = times_transpose("back0", early[4 * half :], slab_weight)
    late = residual_of(LATE, (2, 4), own, theirs)
    back_b = times_transpose("back_b", late, slab_weight)
    far_low = hop(back_b[:half], 2, 1)
    low_from3 = hop(back_b[half:], 2, 3)
    top_from1 = hop(back1[:half], 2, 1)
    top_from3 = hop(plus(back_a[half:], far_top), 2, 3)
    low_from1 = hop(plus(back1[half:], far_low), 2, 1)

    pieces = [top2, top3, top1, low1, groups[0], low2, low3]
    slab_grad, first = None, 0
    for count in SLAB_CUTS:
        slab_grad = slab_product(pieces, early, late, slab_grad, first, count)
        first += count

    upper = back0[:half] + top_from1.astype(jnp.float32) + top_from3.astype(jnp.float32)
    mid = half // 2
    piece = upper[mid:].astype(jnp.bfloat16)
    own_part, piece, low0 = lax.optimization_barrier((upper[:mid], piece, back0[half:]))
    folded = hop(piece, 1, 1)
    lower = low0 + low_from1.astype(jnp.float32) + low_from3.astype(jnp.float32)
    total = own_part + folded.astype(jnp.float32)
    for k in (2, 3):
        piece = lower[(k - 2) * mid : (k - 1) * mid].astype(jnp.bfloat16)
        total = total + hop(piece, 1, k).astype(jnp.float32)
    cut = total.reshape(4, -1, total.shape[-1])
    total = cut[0]
    for k in (1, 2, 3):
        total = total + hop(cut[k].astype(jnp.bfloat16), 0, k).astype(jnp.float32)
    return total, slab_grad


def solution(mesh):
    placed = (P("col", "row"), P("row", "col"), P(None, "col"), P(), P())
    return jax.shard_map(
        body,
        mesh=mesh,
        in_specs=placed,
        out_specs=(P("col", "row"), P("row", "col")),
        check_vma=False,
    )
```
